32 devices in a mesh: grp: 8 (over z, y), dev: 4 (over x, core).
Axes of the slice: x: 2, y: 2, z: 4, core: 2. Of those that a mesh axis runs over, the one named last changes fastest.
Arguments:
- right_side: float32 [8, 4, 3, 4096], P('grp', 'dev'), may hold values from -15 to 15
- elem_nodes: int32 [8, 4, 27, 512], P('grp', 'dev'), may hold values from 0 to 4095, as said below
- elem_coef: float32 [8, 4, 512], P('grp', 'dev'), may hold values from 0.2 to 5
- node_mass: float32 [8, 4, 3, 4096], P('grp', 'dev'), may hold values from 0.5 to 4
- face_slots: int32 [8, 4, 4, 512], P('grp', 'dev'), may hold values from 0 to 4096, as said below
- coarse_nodes: int32 [8, 4, 4, 4096], P('grp', 'dev'), may hold values from 0 to 1535, as said below
- coarse_weights: float32 [8, 4, 4, 4096], P('grp', 'dev'), may hold values from 0.1 to 0.6
- elem_matrix: float32 [81, 81], replicated, may hold values from -1 to 2, as said below
- chol_inverse: float32 [4608, 4608], P('dev'), may hold values from -1 to 1, as said below
Outputs:
- preconditioned: float32 [8, 4, 3, 4096], P('grp', 'dev')
The draws below stay inside these ranges and needn't reach their ends.
Inputs may be any that keep to these rules, and one draw needn't show every extreme that they name: `elem_nodes`: the 27 entries of one element are distinct. `face_slots`: an entry 4096 is padding; the other entries of one subdomain are distinct. Slot p of a face and slot p of the neighbour's face back name the same shared node: both are padding or neither. Live slots come first in a face; faces with no neighbour subdomain are all padding; some face has all 512 slots live. `coarse_nodes`: the entries of subdomain (g, d) lie in the 64 coarse nodes from ((4 * g + d) * 1536) // 32 on, counted modulo 1536. `elem_matrix`: Symmetric; each diagonal entry is positive and exceeds the sum of the magnitudes of the other entries of its row. `chol_inverse`: lower triangular with a positive diagonal.
All inputs are finite; a program needn't handle non-finite values.
Results may differ from the reference program's by a relative error of at most 0.0001.
Values sent between devices are 32-bit elements; how exact they have to be, the bound alone decides.
No kernel may reach another device: no remote copies, remote signals or barrier semaphores. Data moves between devices by JAX's collectives and lax.ppermute only.
A program may use at most 128 MiB of HBM per device.

```python
import math
from functools import partial
import jax
import jax.numpy as jnp
from jax import lax

ELEM = 512
FACE = 512
CN = 1536
PRE = 2
POST = 2
NL = 4096
NC = 4608
N_GRP = 8
N_DEV = 4


def draw_elem_nodes(key, part):
    key_base, key_step = jax.random.split(jax.random.fold_in(key, 3))
    first = jax.random.randint(key_base, (N_GRP, N_DEV, 1, ELEM), 0, NL)
    stride = jax.random.randint(key_step, (N_GRP, N_DEV, 1, ELEM), 1, NL // 32 + 1)
    offset = jnp.arange(27, dtype=jnp.int32)[None, None, :, None]
    return ((first + offset * stride) % NL).astype(jnp.int32)


def draw_face_slots(key, part):
    key_perm, key_grp, key_dev = jax.random.split(jax.random.fold_in(key, 11), 3)
    subkeys = jax.random.split(key_perm, N_GRP * N_DEV)

    def pick_slots(subkey):
        return jax.random.permutation(subkey, NL)[:4 * FACE]
    chosen = jax.vmap(pick_slots)(subkeys).reshape(N_GRP, N_DEV, 4, FACE).astype(jnp.int32)
    grp_live = jax.random.randint(key_grp, (N_GRP + 1, N_DEV), FACE // 2, FACE + 1)
    grp_live = grp_live.at[1, 0].set(FACE)
    grp_row = jnp.arange(N_GRP + 1)[:, None]
    grp_live = jnp.where((grp_row == 0) | (grp_row == N_GRP), 0, grp_live)
    dev_live = jax.random.randint(key_dev, (N_GRP, N_DEV + 1), FACE // 2, FACE + 1)
    dev_col = jnp.arange(N_DEV + 1)[None, :]
    dev_live = jnp.where((dev_col == 0) | (dev_col == N_DEV), 0, dev_live)
    counts = jnp.stack([grp_live[:-1], grp_live[1:], dev_live[:, :-1], dev_live[:, 1:]], axis=2)
    slot_number = jnp.arange(FACE)[None, None, None, :]
    return jnp.where(slot_number < counts[..., None], chosen, NL).astype(jnp.int32)


def draw_coarse_nodes(key, part):
    device = jnp.arange(N_GRP * N_DEV, dtype=jnp.int32).reshape(N_GRP, N_DEV, 1, 1)
    home = device * CN // (N_GRP * N_DEV)
    spread = jax.random.randint(jax.random.fold_in(key, 23), (N_GRP, N_DEV, 4, NL), 0, 64)
    return ((home + spread) % CN).astype(jnp.int32)


def draw_elem_matrix(key, part):
    key_off, key_diag = jax.random.split(jax.random.fold_in(key, 5))
    raw = 0.012 * jax.random.normal(key_off, (81, 81), jnp.float32)
    upper = jnp.triu(raw, 1)
    offdiag = upper + upper.T
    dominant = 1.25 * jnp.sum(jnp.abs(offdiag), axis=1) + jax.random.uniform(key_diag, (81,), jnp.float32, 0.1, 0.4)
    return offdiag + jnp.diag(dominant)


def draw_chol_inverse(key, part):
    key_off, key_diag = jax.random.split(jax.random.fold_in(key, 7))
    raw = 0.06 * jax.random.normal(key_off, (NC, NC), jnp.float32) / jnp.sqrt(1.0 * NC)
    diagonal = jax.random.uniform(key_diag, (NC,), jnp.float32, 0.1, 0.2)
    return jnp.tril(raw, -1) + jnp.diag(diagonal)


def levels(stream_key, shape, cuts, least, largest):
    factor_of = 1.0
    for position, parts in cuts:
        steps = jax.random.uniform(jax.random.fold_in(jax.random.fold_in(stream_key, 6), position), (parts,), jnp.float32, least / len(cuts), largest / len(cuts))
        factor_of = factor_of * jnp.repeat(jnp.exp(steps), shape[position] // parts).reshape((-1,) + (1,) * (len(shape) - 1 - position))
    return factor_of


def bell_draw(key, extent, scale, reach, cuts=(), kind=jnp.bfloat16):
    array = jax.random.normal(key, extent, jnp.float32) * scale
    if len(cuts) > 0:
        array = levels(key, extent, cuts, -0.22, 0.18) * array
    return jnp.clip(array, min=-reach, max=reach).astype(kind)


def setup_inputs(seed: int = 0) -> dict:
    seeds = jax.random.split(jax.random.key(seed), 10)
    return {
        "right_side": bell_draw(seeds[0], (N_GRP, N_DEV, 3, NL), 3.0, 15.0, ((0, 8), (1, 4)), jnp.float32),
        "elem_nodes": draw_elem_nodes(jax.random.fold_in(seeds[9], 71), 0),
        "elem_coef": jnp.clip(jnp.exp(math.log(5.0) - 3.218876 * jax.random.uniform(seeds[2], (N_GRP, N_DEV, ELEM), jnp.float32) ** levels(seeds[2], (N_GRP, N_DEV, ELEM), ((0, 8), (1, 4)), -0.2, 0.2)), 0.2, 5.0),
        "node_mass": jnp.clip(jnp.exp(math.log(4.0) - 2.0794415 * jax.random.uniform(seeds[3], (N_GRP, N_DEV, 3, NL), jnp.float32) ** levels(seeds[3], (N_GRP, N_DEV, 3, NL), ((0, 8), (1, 4)), -0.2, 0.2)), 0.5, 4.0),
        "face_slots": draw_face_slots(jax.random.fold_in(seeds[9], 71), 0),
        "coarse_nodes": draw_coarse_nodes(jax.random.fold_in(seeds[9], 71), 0),
        "coarse_weights": jnp.clip(0.1 + 0.5 * jax.random.uniform(seeds[6], (N_GRP, N_DEV, 4, NL), jnp.float32) ** levels(seeds[6], (N_GRP, N_DEV, 4, NL), ((0, 8), (1, 4)), -0.2, 0.2), 0.1, 0.6),
        "elem_matrix": draw_elem_matrix(jax.random.fold_in(seeds[9], 71), 0),
        "chol_inverse": draw_chol_inverse(jax.random.fold_in(seeds[9], 71), 0),
    }


DAMPING = 0.6
PRECISE = lax.Precision.HIGHEST


def over_devices(function, arrays):
    def mapped(row_arrays):
        return jax.vmap(function)(*row_arrays)
    return lax.map(mapped, arrays)


def element_apply(matrix, field, node_index, elem_scale, mass_here):
    elem_count = node_index.shape[1]
    gathered = field[:, node_index].reshape(81, elem_count)
    product = jnp.dot(matrix, gathered, precision=PRECISE) * elem_scale[None, :]
    summed = jnp.zeros_like(field).at[:, node_index].add(product.reshape(3, 27, elem_count))
    return summed + mass_here * field


def local_diagonal(main_diag, node_index, elem_scale, mass_here):
    summed = jnp.zeros_like(mass_here).at[:, node_index].add(main_diag[:, :, None] * elem_scale[None, None, :])
    return summed + mass_here


def face_values(field, face_index):
    return field.at[:, face_index].get(mode="fill", fill_value=0.0)


def add_received(field, face_index, received):
    return field.at[:, face_index].add(received, mode="drop")


def assemble(field, face_slots):
    outgoing = over_devices(face_values, (field, face_slots))
    zero_grp = jnp.zeros_like(outgoing[:1, :, :, 0])
    from_below = jnp.concatenate([zero_grp, outgoing[:-1, :, :, 1]], axis=0)
    from_above = jnp.concatenate([outgoing[1:, :, :, 0], zero_grp], axis=0)
    zero_dev = jnp.zeros_like(outgoing[:, :1, :, 0])
    from_left = jnp.concatenate([zero_dev, outgoing[:, :-1, :, 3]], axis=1)
    from_right = jnp.concatenate([outgoing[:, 1:, :, 2], zero_dev], axis=1)
    received = jnp.stack([from_below, from_above, from_left, from_right], axis=3)
    return over_devices(add_received, (field, face_slots, received))


def restrict(coarse_width, field, coarse_index, weights):
    values = weights[None] * field[:, None, :]
    return jnp.zeros((3, coarse_width), field.dtype).at[:, coarse_index].add(values).reshape(3 * coarse_width)


def prolong(coarse, coarse_index, weights):
    coarse_table = coarse.reshape(3, coarse.shape[0] // 3)
    return jnp.sum(weights[None] * coarse_table[:, coarse_index], axis=1)


def reference(right_side, elem_nodes, elem_coef, node_mass, face_slots, coarse_nodes, coarse_weights, elem_matrix, chol_inverse):
    main_diag = jnp.diagonal(elem_matrix).reshape(3, 27)

    def operate(field):
        local = over_devices(partial(element_apply, elem_matrix), (field, elem_nodes, elem_coef, node_mass))
        return assemble(local, face_slots)

    local_diag = over_devices(partial(local_diagonal, main_diag), (elem_nodes, elem_coef, node_mass))
    diag_total = assemble(local_diag, face_slots)
    iterate = DAMPING * right_side / diag_total
    for sweep_index in range(PRE - 1):
        iterate = iterate + DAMPING * (right_side - operate(iterate)) / diag_total
    residual = right_side - operate(iterate)
    pieces = over_devices(partial(restrict, CN), (residual, coarse_nodes, coarse_weights))
    coarse_rhs = jnp.sum(pieces, axis=(0, 1))
    halfway = jnp.dot(chol_inverse, coarse_rhs, precision=PRECISE)
    correction = jnp.dot(halfway, chol_inverse, precision=PRECISE)
    iterate = iterate + over_devices(partial(prolong, correction), (coarse_nodes, coarse_weights))
    for sweep_index in range(POST):
        iterate = iterate + DAMPING * (right_side - operate(iterate)) / diag_total
    return iterate
```

```python
import jax
import jax.numpy as jnp
from jax import lax
from jax.experimental import pallas as pl
from jax.experimental.pallas import tpu as pltpu
from jax.sharding import PartitionSpec as P

POST = 2
DAMPING = 0.6
WINDOW = 64
LANES = 128
F32 = jnp.float32
BF16 = jnp.bfloat16


def two_parts(value):
    high = value.astype(BF16)
    low = (value - high.astype(F32)).astype(BF16)
    return high, low


def nt_dot(left, right):
    return lax.dot_general(left, right, (((1,), (1,)), ((), ())), preferred_element_type=F32)


def low_onehot(index_row):
    low = index_row & (LANES - 1)
    rows = lax.broadcasted_iota(jnp.int32, (LANES, index_row.shape[1]), 0)
    return jnp.where(rows == low, 1.0, 0.0).astype(BF16)


def high_mask(index_row, count):
    rows = lax.broadcasted_iota(jnp.int32, (count, index_row.shape[1]), 0)
    return rows == (index_row >> 7)


def field_parts(field):
    high, low = two_parts(field)
    return jnp.concatenate([high, low], axis=1)


def gather_slot(parts, index_row):
    count = parts.shape[0] // 3
    onehot = low_onehot(index_row)
    picked = jnp.dot(parts, jnp.concatenate([onehot, onehot], axis=0), preferred_element_type=F32)
    mask = high_mask(index_row, count)
    return [
        jnp.sum(jnp.where(mask, picked[c * count:(c + 1) * count], 0.0), axis=0, keepdims=True)
        for c in range(3)
    ]


def scatter_slot(rows_high, rows_low, index_row, count):
    mask = high_mask(index_row, count)
    spread = [
        jnp.where(mask, row, 0.0).astype(BF16)
        for row in rows_high + rows_low
    ]
    return nt_dot(jnp.concatenate(spread, axis=0), low_onehot(index_row))


def join_parts(total):
    half = total.shape[0] // 2
    return total[:half] + total[half:]


def slot_rows(par_ref):
    grp_odd = par_ref[0]
    dev_odd = par_ref[1]
    return [1 - grp_odd, grp_odd, 3 - dev_odd, 2 + dev_odd]


def send_faces(field, faces_ref, par_ref, out_refs):
    parts = field_parts(field)
    for slot, face in enumerate(slot_rows(par_ref)):
        rows = gather_slot(parts, faces_ref[pl.ds(face, 1), :])
        out_refs[slot][...] = jnp.concatenate(rows, axis=0)


def add_faces(faces_ref, par_ref, in_refs, count):
    total = None
    for slot, face in enumerate(slot_rows(par_ref)):
        value = in_refs[slot][...]
        high = value.astype(BF16).astype(F32)
        low = value - high
        got = scatter_slot(
            [high[c:c + 1] for c in range(3)],
            [low[c:c + 1] for c in range(3)],
            faces_ref[pl.ds(face, 1), :],
            count,
        )
        total = got if total is None else total + got
    return join_parts(total)


def scatter_elements(high_ref, low_ref, nodes_ref, count):
    local = nodes_ref.shape[0]
    total = None
    for i in range(local):
        got = scatter_slot(
            [high_ref[c * local + i:c * local + i + 1, :] for c in range(3)],
            [low_ref[c * local + i:c * local + i + 1, :] for c in range(3)],
            nodes_ref[i:i + 1, :],
            count,
        )
        total = got if total is None else total + got
    return join_parts(total)


def store_parts(value, high_ref, low_ref):
    high = value.astype(BF16).astype(F32)
    high_ref[...] = high
    low_ref[...] = value - high


def element_apply(field, nodes_ref, coef_ref, matrix_ref, mat_s, got_s, high_s, low_s):
    count = field.shape[0] // 3
    local = nodes_ref.shape[0]
    size = matrix_ref.shape[0]
    mat_s[...] = jnp.zeros_like(mat_s)
    mat_s[:size, :size] = matrix_ref[...]
    parts = field_parts(field)
    got_s[80:, :] = jnp.zeros_like(got_s[80:, :])
    for i in range(local):
        rows = gather_slot(parts, nodes_ref[i:i + 1, :])
        for c in range(3):
            got_s[c * local + i:c * local + i + 1, :] = rows[c]
    mat_high, mat_low = two_parts(mat_s[...])
    got_high, got_low = two_parts(got_s[...])
    product = (
        jnp.dot(mat_high, got_high, preferred_element_type=F32)
        + jnp.dot(mat_high, got_low, preferred_element_type=F32)
        + jnp.dot(mat_low, got_high, preferred_element_type=F32)
    )
    store_parts(product * coef_ref[...], high_s, low_s)
    return scatter_elements(high_s, low_s, nodes_ref, count)


def diag_kernel(par, nodes, coef, mass, faces, matrix, diag_out, s0, s1, s2, s3, high_s, low_s):
    size = matrix.shape[0]
    rows = lax.broadcasted_iota(jnp.int32, (size, size), 0)
    cols = lax.broadcasted_iota(jnp.int32, (size, size), 1)
    main = jnp.sum(jnp.where(rows == cols, matrix[...], 0.0), axis=1, keepdims=True)
    value = main * coef[...]
    high = value.astype(BF16).astype(F32)
    high_s[:size, :] = high
    low_s[:size, :] = value - high
    diag = mass[...] + scatter_elements(high_s, low_s, nodes, mass.shape[0] // 3)
    diag_out[...] = diag
    send_faces(diag, faces, par, (s0, s1, s2, s3))


def first_kernel(par, diag, g0, g1, g2, g3, right, nodes, coef, mass, faces, matrix,
                 gain_out, field_out, local_out, s0, s1, s2, s3, mat_s, got_s, high_s, low_s):
    count = mass.shape[0] // 3
    total = diag[...] + add_faces(faces, par, (g0, g1, g2, g3), count)
    gain = DAMPING / total
    gain_out[...] = gain
    field = gain * right[...]
    field_out[...] = field
    local = mass[...] * field + element_apply(field, nodes, coef, matrix, mat_s, got_s, high_s, low_s)
    local_out[...] = local
    send_faces(local, faces, par, (s0, s1, s2, s3))


def sweep_kernel(par, local_in, g0, g1, g2, g3, field_in, gain, right, nodes, coef, mass, faces, matrix,
                 field_out, local_out, s0, s1, s2, s3, mat_s, got_s, high_s, low_s):
    count = mass.shape[0] // 3
    total = local_in[...] + add_faces(faces, par, (g0, g1, g2, g3), count)
    field = field_in[...] + gain[...] * (right[...] - total)
    field_out[...] = field
    local = mass[...] * field + element_apply(field, nodes, coef, matrix, mat_s, got_s, high_s, low_s)
    local_out[...] = local
    send_faces(local, faces, par, (s0, s1, s2, s3))


def last_kernel(par, local_in, g0, g1, g2, g3, field_in, gain, right, faces, field_out):
    count = right.shape[0] // 3
    total = local_in[...] + add_faces(faces, par, (g0, g1, g2, g3), count)
    field_out[...] = field_in[...] + gain[...] * (right[...] - total)


def transfer_matrix(home, width, coarse, weights):
    total = None
    for q in range(coarse.shape[0]):
        offset = coarse[q:q + 1, :] - home
        offset = jnp.where(offset < 0, offset + width, offset)
        rows = lax.broadcasted_iota(jnp.int32, (WINDOW, coarse.shape[1]), 0)
        part = jnp.where(rows == offset, weights[q:q + 1, :], 0.0)
        total = part if total is None else total + part
    return total


def prepare_kernel(width, par, coarse, weights, high_out, low_out):
    high, low = two_parts(transfer_matrix(par[2], width, coarse, weights))
    high_out[...] = high
    low_out[...] = low


def restrict_kernel(par, local_in, g0, g1, g2, g3, right, faces, high_in, low_in, out, res_s, flat_s):
    count = right.shape[0] // 3
    total = local_in[...] + add_faces(faces, par, (g0, g1, g2, g3), count)
    res_s[...] = right[...] - total
    flat_s[...] = jnp.zeros_like(flat_s)
    for h in range(count):
        for c in range(3):
            flat_s[c:c + 1, h * LANES:(h + 1) * LANES] = res_s[c * count + h:c * count + h + 1, :]
    high, low = two_parts(flat_s[...])
    out[...] = nt_dot(high, high_in[...]) + nt_dot(low, high_in[...]) + nt_dot(high, low_in[...])


def prolong_kernel(par, window, field_in, nodes, coef, mass, faces, matrix, high_in, low_in,
                   field_out, local_out, s0, s1, s2, s3, mat_s, got_s, high_s, low_s, flat_s, res_s):
    count = mass.shape[0] // 3
    high, low = two_parts(window[...])
    flat_s[...] = (
        jnp.dot(high, high_in[...], preferred_element_type=F32)
        + jnp.dot(low, high_in[...], preferred_element_type=F32)
        + jnp.dot(high, low_in[...], preferred_element_type=F32)
    )
    for h in range(count):
        for c in range(3):
            res_s[c * count + h:c * count + h + 1, :] = flat_s[c:c + 1, h * LANES:(h + 1) * LANES]
    field = field_in[...] + res_s[...]
    field_out[...] = field
    local = mass[...] * field + element_apply(field, nodes, coef, matrix, mat_s, got_s, high_s, low_s)
    local_out[...] = local
    send_faces(local, faces, par, (s0, s1, s2, s3))


def coarse_kernel(rhs, factor, out):
    @pl.when(pl.program_id(0) == 0)
    def _():
        out[...] = jnp.zeros_like(out)

    block = factor[...]
    half = jnp.sum(block * rhs[...], axis=1, keepdims=True)
    out[...] += jnp.sum(block * half, axis=0, keepdims=True)


def local_program(mesh_shape, right_side, elem_nodes, elem_coef, node_mass, face_slots, coarse_nodes,
                  coarse_weights, elem_matrix, chol_inverse):
    n_grp, n_dev = mesh_shape
    nodes_count = right_side.shape[-1]
    hi = nodes_count // LANES
    local_nodes, elements = elem_nodes.shape[2:]
    slots = face_slots.shape[-1]
    width = chol_inverse.shape[1] // 3
    stride = width // (n_grp * n_dev)
    grp = lax.axis_index("grp")
    dev = lax.axis_index("dev")
    home = (grp * n_dev + dev) * width // (n_grp * n_dev)
    par = jnp.stack([grp & 1, dev & 1, home, dev]).astype(jnp.int32)

    right = right_side.reshape(3 * hi, LANES)
    mass = node_mass.reshape(3 * hi, LANES)
    nodes = elem_nodes[0, 0]
    coef = elem_coef[0]
    faces = face_slots[0, 0]
    coarse = coarse_nodes[0, 0]
    weights = coarse_weights[0, 0]

    smem = pl.BlockSpec(memory_space=pltpu.SMEM)
    vmem = pl.BlockSpec(memory_space=pltpu.VMEM)
    field_t = jax.ShapeDtypeStruct((3 * hi, LANES), F32)
    face_t = [jax.ShapeDtypeStruct((3, slots), F32)] * 4
    rows = 3 * local_nodes
    padded = -(-rows // LANES) * LANES
    part_rows = -(-rows // 16) * 16
    parts_s = [pltpu.VMEM((part_rows, elements), F32)] * 2
    apply_s = [pltpu.VMEM((part_rows, padded), F32), pltpu.VMEM((padded, elements), F32)] + parts_s
    flat_s = pltpu.VMEM((8, nodes_count), F32)

    def call(kernel, outs, scratch, *args):
        return pl.pallas_call(
            kernel,
            out_shape=outs,
            in_specs=[smem] + [vmem] * (len(args) - 1),
            out_specs=jax.tree.map(lambda _: vmem, outs),
            scratch_shapes=scratch,
        )(*args)

    def pairs(axis, parity):
        count = lax.axis_size(axis)
        out = []
        for first in range(parity, count + parity, 2):
            a, b = first % count, (first + 1) % count
            out += [(a, b), (b, a)]
        return out

    def swap(faces_out):
        return [
            lax.ppermute(faces_out[0], "grp", pairs("grp", 0)),
            lax.ppermute(faces_out[1], "grp", pairs("grp", 1)),
            lax.ppermute(faces_out[2], "dev", pairs("dev", 0)),
            lax.ppermute(faces_out[3], "dev", pairs("dev", 1)),
        ]

    transfer_t = jax.ShapeDtypeStruct((WINDOW, nodes_count), BF16)

    def prepare(*refs):
        prepare_kernel(width, *refs)

    high_t, low_t = call(prepare, [transfer_t] * 2, [], par, coarse, weights)
    diag, *out = call(diag_kernel, [field_t] + face_t, parts_s, par, nodes, coef, mass, faces, elem_matrix)
    got = swap(out)
    gain, field, local, *out = call(
        first_kernel, [field_t] * 3 + face_t, apply_s,
        par, diag, *got, right, nodes, coef, mass, faces, elem_matrix)
    got = swap(out)
    field, local, *out = call(
        sweep_kernel, [field_t] * 2 + face_t, apply_s,
        par, local, *got, field, gain, right, nodes, coef, mass, faces, elem_matrix)
    got = swap(out)
    window = call(
        restrict_kernel, jax.ShapeDtypeStruct((8, WINDOW), F32), [pltpu.VMEM((3 * hi, LANES), F32), flat_s],
        par, local, *got, right, faces, high_t, low_t)

    total = n_grp * n_dev
    sent = jnp.broadcast_to(window[None, :3], (total, 3, WINDOW))
    windows = lax.all_to_all(sent, ("grp", "dev"), 0, 0)
    pieces = jnp.zeros((total, 3, stride), F32)
    for step in range(-(-WINDOW // stride)):
        piece = windows[:, :, step * stride:(step + 1) * stride]
        piece = jnp.pad(piece, ((0, 0), (0, 0), (0, stride - piece.shape[2])))
        pieces = pieces + jnp.roll(piece, step, axis=0)
    rhs = pieces.transpose(1, 0, 2).reshape(1, 3 * width)

    block = chol_inverse.shape[0]
    while block % 16 == 0 and block > 144:
        block //= 2
    part = pl.pallas_call(
        coarse_kernel,
        grid=(chol_inverse.shape[0] // block,),
        out_shape=jax.ShapeDtypeStruct((1, 3 * width), F32),
        in_specs=[
            pl.BlockSpec((1, 3 * width), lambda i: (0, 0)),
            pl.BlockSpec((block, 3 * width), lambda i: (i, 0)),
        ],
        out_specs=pl.BlockSpec((1, 3 * width), lambda i: (0, 0)),
    )(rhs, chol_inverse)
    table = part.reshape(3, width)
    table = jnp.concatenate([table, table[:, :n_dev * stride + WINDOW]], axis=1)

    def window_of(other):
        return lax.dynamic_slice(table, (0, (grp * n_dev + other) * stride), (3, WINDOW))

    correction = window_of(dev)
    for step in range(1, n_dev):
        correction = correction + lax.ppermute(
            window_of(dev ^ step), "dev", [(i, i ^ step) for i in range(n_dev)])
    correction = jnp.pad(correction, ((0, 5), (0, 0)))

    field, local, *out = call(
        prolong_kernel, [field_t] * 2 + face_t, apply_s + [flat_s, pltpu.VMEM((3 * hi, LANES), F32)],
        par, correction, field, nodes, coef, mass, faces, elem_matrix, high_t, low_t)
    for _ in range(POST - 1):
        got = swap(out)
        field, local, *out = call(
            sweep_kernel, [field_t] * 2 + face_t, apply_s,
            par, local, *got, field, gain, right, nodes, coef, mass, faces, elem_matrix)
    got = swap(out)
    field = call(last_kernel, field_t, [], par, local, *got, field, gain, right, faces)
    return field.reshape(1, 1, 3, nodes_count)


def solution(mesh):
    mesh_shape = (mesh.shape["grp"], mesh.shape["dev"])

    def local(*args):
        return local_program(mesh_shape, *args)

    return jax.shard_map(
        local,
        mesh=mesh,
        in_specs=(
            P("grp", "dev", None, None),
            P("grp", "dev", None, None),
            P("grp", "dev", None),
            P("grp", "dev", None, None),
            P("grp", "dev", None, None),
            P("grp", "dev", None, None),
            P("grp", "dev", None, None),
            P(),
            P("dev", None),
        ),
        out_specs=P("grp", "dev", None, None),
        check_vma=False,
    )
```

```python
import jax
import jax.numpy as jnp
from jax import lax
from jax.experimental import pallas as pl
from jax.experimental.pallas import tpu as pltpu
from jax.sharding import PartitionSpec as P

POST = 2
DAMPING = 0.6
WINDOW = 64
LANES = 128
BIG = 16
CHUNKS = 9
F32 = jnp.float32
BF16 = jnp.bfloat16


def two_parts(value):
    high = value.astype(BF16)
    low = (value - high.astype(F32)).astype(BF16)
    return high, low


def nt_dot(left, right):
    return lax.dot_general(left, right, (((1,), (1,)), ((), ())), preferred_element_type=F32)


def low_onehot(index_row):
    low = index_row & (LANES - 1)
    rows = lax.broadcasted_iota(jnp.int32, (LANES, index_row.shape[1]), 0)
    return jnp.where(rows == low, 1.0, 0.0).astype(BF16)


def high_onehot(index_row, count):
    rows = lax.broadcasted_iota(jnp.int32, (count, index_row.shape[1]), 0)
    return jnp.where(rows == (index_row >> 7), 1.0, 0.0).astype(BF16)


def field_parts(field):
    high, low = two_parts(field)
    return jnp.concatenate([high, low], axis=1)


def gather_slot(parts, onehot, index_row):
    count = parts.shape[0] // 3
    picked = jnp.dot(parts, jnp.concatenate([onehot, onehot], axis=0), preferred_element_type=F32)
    rows = lax.broadcasted_iota(jnp.int32, (count, index_row.shape[1]), 0)
    mask = rows == (index_row >> 7)
    return [
        jnp.sum(jnp.where(mask, picked[c * count:(c + 1) * count], 0.0), axis=0, keepdims=True)
        for c in range(3)
    ]


def scatter_slot(rows, low_hot, high_hot):
    spread = []
    for row in rows:
        wide = jnp.broadcast_to(row, (16, row.shape[1])).astype(BF16)
        spread.append(jnp.concatenate([wide] * (high_hot.shape[0] // 16), axis=0) * high_hot)
    return nt_dot(jnp.concatenate(spread, axis=0), low_hot)


def join_parts(total):
    half = total.shape[0] // 2
    return total[:half] + total[half:]


def send_faces(field, first, index, low_hot, out_refs):
    parts = field_parts(field)
    for slot in range(4):
        rows = gather_slot(parts, low_hot[first + slot], index[first + slot:first + slot + 1, :])
        out_refs[slot][...] = jnp.concatenate(rows, axis=0)


def add_faces(first, low_hot, high_hot, in_refs):
    total = None
    for slot in range(4):
        value = in_refs[slot][...]
        high = value.astype(BF16).astype(F32)
        low = value - high
        rows = [part[c:c + 1] for part in (high, low) for c in range(3)]
        got = scatter_slot(rows, low_hot[first + slot], high_hot[first + slot])
        total = got if total is None else total + got
    return join_parts(total)


def scatter_elements(high_s, low_s, first, low_hot, high_hot):
    total = None
    for i in range(first):
        rows = [
            part[c * first + i:c * first + i + 1, :]
            for part in (high_s, low_s) for c in range(3)
        ]
        got = scatter_slot(rows, low_hot[i], high_hot[i])
        total = got if total is None else total + got
    return join_parts(total)


def store_parts(value, high_s, low_s):
    high = value.astype(BF16).astype(F32)
    high_s[...] = high
    low_s[...] = value - high


def element_apply(field, mesh_refs, scratch):
    index, coef, mat_high, mat_low, low_hot, high_hot = mesh_refs
    got_s, high_s, low_s = scratch
    first = low_hot.shape[0] - 4
    parts = field_parts(field)
    got_s[80:, :] = jnp.zeros_like(got_s[80:, :])
    for i in range(first):
        rows = gather_slot(parts, low_hot[i], index[i:i + 1, :])
        for c in range(3):
            got_s[c * first + i:c * first + i + 1, :] = rows[c]
    got_high, got_low = two_parts(got_s[...])
    product = (
        jnp.dot(mat_high[...], got_high, preferred_element_type=F32)
        + jnp.dot(mat_high[...], got_low, preferred_element_type=F32)
        + jnp.dot(mat_low[...], got_high, preferred_element_type=F32)
    )
    store_parts(product * coef[...], high_s, low_s)
    return scatter_elements(high_s, low_s, first, low_hot, high_hot)


def finish_apply(field, mass, mesh_refs, scratch, local_out, faces_out):
    local = mass[...] * field + element_apply(field, mesh_refs, scratch)
    local_out[...] = local
    index, low_hot = mesh_refs[0], mesh_refs[4]
    send_faces(local, low_hot.shape[0] - 4, index, low_hot, faces_out)


def diag_kernel(par, nodes_h, coef_h, mass_h, right_h, faces_h, matrix_h,
                diag_out, s0, s1, s2, s3, index, coef, mass, right, mat_high, mat_low, low_hot, high_hot,
                nodes_s, faces_s, matrix_s, pad_s, high_s, low_s, sems):
    moves = [(nodes_h, nodes_s), (coef_h, coef), (mass_h, mass), (right_h, right),
             (faces_h, faces_s), (matrix_h, matrix_s)]
    copies = [pltpu.make_async_copy(src, dst, sems.at[n]) for n, (src, dst) in enumerate(moves)]
    for copy in copies:
        copy.start()
    first = low_hot.shape[0] - 4
    count = high_hot.shape[1]
    size = matrix_h.shape[0]
    pad_s[...] = jnp.zeros_like(pad_s)
    copies[0].wait()
    for i in range(first):
        for t in range(nodes_s.shape[1]):
            index[i:i + 1, t * LANES:(t + 1) * LANES] = nodes_s[i, t:t + 1, :]
    copies[4].wait()
    for slot, face in enumerate([1 - par[0], par[0], 3 - par[1], 2 + par[1]]):
        index[first + slot:first + slot + 1, :] = faces_s[pl.ds(face, 1), :]
    copies[5].wait()
    pad_s[:size, :size] = matrix_s[...]
    mat_high[...], mat_low[...] = two_parts(pad_s[...])
    rows = lax.broadcasted_iota(jnp.int32, pad_s.shape, 0)
    cols = lax.broadcasted_iota(jnp.int32, pad_s.shape, 1)
    main = jnp.sum(jnp.where(rows == cols, pad_s[...], 0.0), axis=1, keepdims=True)
    copies[1].wait()
    store_parts(main * coef[...], high_s, low_s)
    total = None
    for i in range(first + 4):
        row = index[i:i + 1, :]
        low = low_onehot(row)
        high = high_onehot(row, count)
        low_hot[i] = low
        high_hot[i] = high
        if i < first:
            rows = [
                part[c * first + i:c * first + i + 1, :]
                for part in (high_s, low_s) for c in range(3)
            ]
            got = scatter_slot(rows, low, high)
            total = got if total is None else total + got
    copies[2].wait()
    diag = mass[...] + join_parts(total)
    diag_out[...] = diag
    send_faces(diag, first, index, low_hot, (s0, s1, s2, s3))
    copies[3].wait()


def first_kernel(diag, g0, g1, g2, g3, mass, right, index, coef, mat_high, mat_low, low_hot, high_hot,
                 gain_out, field_out, local_out, s0, s1, s2, s3, *scratch):
    total = diag[...] + add_faces(low_hot.shape[0] - 4, low_hot, high_hot, (g0, g1, g2, g3))
    gain = DAMPING / total
    gain_out[...] = gain
    field = gain * right[...]
    field_out[...] = field
    finish_apply(field, mass, (index, coef, mat_high, mat_low, low_hot, high_hot), scratch,
                 local_out, (s0, s1, s2, s3))


def sweep_kernel(local_in, g0, g1, g2, g3, field_in, gain, mass, right, index, coef, mat_high, mat_low,
                 low_hot, high_hot, field_out, local_out, s0, s1, s2, s3, *scratch):
    total = local_in[...] + add_faces(low_hot.shape[0] - 4, low_hot, high_hot, (g0, g1, g2, g3))
    field = field_in[...] + gain[...] * (right[...] - total)
    field_out[...] = field
    finish_apply(field, mass, (index, coef, mat_high, mat_low, low_hot, high_hot), scratch,
                 local_out, (s0, s1, s2, s3))


def with_move(kernel, n_in, n_out, first_row):
    def moving(*refs):
        source, ins = refs[0], refs[1:1 + n_in]
        outs, target = refs[1 + n_in:1 + n_in + n_out], refs[1 + n_in + n_out]
        scratch, sem = refs[2 + n_in + n_out:-1], refs[-1]
        size = target.shape[0] // CHUNKS

        def chunk(n):
            start = pl.multiple_of(n * size, 8)
            return pltpu.make_async_copy(
                source.at[pl.ds(first_row + start, size), :], target.at[pl.ds(start, size), :], sem.at[n])

        @pl.loop(0, CHUNKS)
        def _(n):
            chunk(n).start()

        kernel(*ins, *outs, *scratch)

        @pl.loop(0, CHUNKS)
        def _(n):
            chunk(n).wait()

    return moving


def last_kernel(local_in, g0, g1, g2, g3, field_in, gain, right, low_hot, high_hot, field_out):
    total = local_in[...] + add_faces(low_hot.shape[0] - 4, low_hot, high_hot, (g0, g1, g2, g3))
    field_out[...] = field_in[...] + gain[...] * (right[...] - total)


def prepare_kernel(width, par, coarse_h, weights_h, table, coarse, weights, sems):
    copies = [pltpu.make_async_copy(coarse_h, coarse, sems.at[0]),
              pltpu.make_async_copy(weights_h, weights, sems.at[1])]
    for copy in copies:
        copy.start()
    for copy in copies:
        copy.wait()
    total = None
    for q in range(coarse.shape[0]):
        offset = coarse[q:q + 1, :] - par[2]
        offset = jnp.where(offset < 0, offset + width, offset)
        rows = lax.broadcasted_iota(jnp.int32, (WINDOW, coarse.shape[1]), 0)
        part = jnp.where(rows == offset, weights[q:q + 1, :], 0.0)
        total = part if total is None else total + part
    high, low = two_parts(total)
    table[:WINDOW, :] = high
    table[WINDOW:, :] = low


def restrict_kernel(local_in, g0, g1, g2, g3, right, low_hot, high_hot, table, out, res_s, flat_s):
    count = high_hot.shape[1]
    total = local_in[...] + add_faces(low_hot.shape[0] - 4, low_hot, high_hot, (g0, g1, g2, g3))
    res_s[...] = right[...] - total
    flat_s[...] = jnp.zeros_like(flat_s)
    for h in range(count):
        for c in range(3):
            flat_s[c:c + 1, h * LANES:(h + 1) * LANES] = res_s[c * count + h:c * count + h + 1, :]
    high, low = two_parts(flat_s[...])
    wide = nt_dot(high, table[...])
    both = wide + pltpu.roll(wide, WINDOW, 1) + nt_dot(low, table[...])
    lanes = lax.broadcasted_iota(jnp.int32, both.shape, 1)
    window = jnp.where(lanes < WINDOW, both, 0.0)[:4]
    for other in range(out.shape[0]):
        out[other] = window


def prolong_kernel(w0, *refs):
    extra = refs[:-22]
    (field_in, table, mass, index, coef, mat_high, mat_low, low_hot, high_hot,
     field_out, local_out, s0, s1, s2, s3, got_s, high_s, low_s, flat_s, res_s, wide_s, low_w) = refs[-22:]
    count = high_hot.shape[1]
    window = w0[...]
    for ref in extra:
        window = window + ref[...]
    high = window.astype(BF16).astype(F32)
    low = window - high
    flat_s[...] = (
        jnp.dot((high + pltpu.roll(high, WINDOW, 1)).astype(BF16), table[...], preferred_element_type=F32)
        + jnp.dot(low.astype(BF16), table[...], preferred_element_type=F32)
    )
    for h in range(count):
        for c in range(3):
            res_s[c * count + h:c * count + h + 1, :] = flat_s[c:c + 1, h * LANES:(h + 1) * LANES]
    field = field_in[...] + res_s[...]
    field_out[...] = field
    finish_apply(field, mass, (index, coef, mat_high, mat_low, low_hot, high_hot), (got_s, high_s, low_s),
                 local_out, (s0, s1, s2, s3))


def coarse_kernel(n_dev, width, par, windows, upper, lower, *refs):
    outs, (rhs_s, half_s) = refs[:n_dev], refs[n_dev:]
    total = windows.shape[0]
    stride = width // total
    tiles = width // LANES
    lanes = lax.broadcasted_iota(jnp.int32, (4, LANES), 1)
    sums = [jnp.zeros((4, LANES), F32)] * tiles
    for other in range(total):
        tile, shift = divmod(other * stride, LANES)
        window = windows[other]
        if shift:
            window = pltpu.roll(window, shift, 1)
        if shift + WINDOW > LANES:
            sums[tile] = sums[tile] + jnp.where(lanes >= shift, window, 0.0)
            after = (tile + 1) % tiles
            sums[after] = sums[after] + jnp.where(lanes < shift, window, 0.0)
        else:
            sums[tile] = sums[tile] + window
    for tile in range(tiles):
        for c in range(3):
            rhs_s[c * tiles + tile] = jnp.broadcast_to(sums[tile][c:c + 1], (8, LANES))
    rows = upper.shape[0]
    block = 64

    def first_product(factor, offset):
        def body(step, carry):
            start = pl.multiple_of(step * block, block)
            acc = [None] * (block // 8)
            for tile in range(3 * tiles):
                value = rhs_s[tile]
                piece = factor[pl.ds(start, block), tile * LANES:(tile + 1) * LANES]
                for r in range(block // 8):
                    term = piece[r * 8:(r + 1) * 8] * value
                    acc[r] = term if acc[r] is None else acc[r] + term
            half_s[pl.ds(offset + start, block), :] = jnp.concatenate(acc, axis=0)
            return carry

        lax.fori_loop(0, rows // block, body, 0)

    first_product(upper, 0)
    first_product(lower, rows)
    half_s[...] = jnp.broadcast_to(jnp.sum(half_s[...], axis=1, keepdims=True), half_s.shape)

    base = par[3] * stride
    first_tile = base // LANES
    rest = base - first_tile * LANES
    span = -(-(LANES - 1 + (n_dev - 1) * stride + WINDOW) // LANES)
    starts = []
    for c in range(3):
        for t in range(span):
            tile = first_tile + t
            tile = jnp.where(tile >= tiles, tile - tiles, tile)
            starts.append(pl.multiple_of((c * tiles + tile) * LANES, LANES))

    def second_product(factor, offset, sums):
        def body(step, acc):
            start = pl.multiple_of(step * block, block)
            half = half_s[pl.ds(offset + start, block), :]
            out = []
            for n, lane in enumerate(starts):
                piece = factor[pl.ds(start, block), pl.ds(lane, LANES)] * half
                value = acc[n]
                for r in range(block // 8):
                    value = value + piece[r * 8:(r + 1) * 8]
                out.append(value)
            return tuple(out)

        return lax.fori_loop(0, rows // block, body, sums)

    acc = tuple(jnp.zeros((8, LANES), F32) for _ in starts)
    acc = second_product(lower, rows, second_product(upper, 0, acc))
    parts = [jnp.sum(value, axis=0, keepdims=True) for value in acc]
    comps = [jnp.concatenate(parts[c * span:(c + 1) * span], axis=1) for c in range(3)]
    table = jnp.concatenate(comps + [jnp.zeros((5, span * LANES), F32)], axis=0)
    lanes = lax.broadcasted_iota(jnp.int32, (8, LANES), 1)
    for step in range(n_dev):
        shift = rest + (par[4] ^ step) * stride
        moved = pltpu.roll(table, span * LANES - shift, 1)[:, :LANES]
        outs[step][...] = jnp.where(lanes < WINDOW, moved, 0.0)


def local_program(mesh_shape, right_side, elem_nodes, elem_coef, node_mass, face_slots, coarse_nodes,
                  coarse_weights, elem_matrix, chol_inverse):
    n_grp, n_dev = mesh_shape
    total = n_grp * n_dev
    nodes_count = right_side.shape[-1]
    hi = nodes_count // LANES
    local_nodes, elements = elem_nodes.shape[2:]
    slots = face_slots.shape[-1]
    width = chol_inverse.shape[1] // 3
    grp = lax.axis_index("grp")
    dev = lax.axis_index("dev")
    home = (grp * n_dev + dev) * width // total
    par = jnp.stack([grp & 1, dev & 1, home, grp * n_dev, dev]).astype(jnp.int32)

    right = right_side.reshape(3 * hi, LANES)
    mass = node_mass.reshape(3 * hi, LANES)
    nodes = elem_nodes.reshape(local_nodes, elements // LANES, LANES)
    coef = elem_coef[0]
    faces = face_slots[0, 0]
    coarse = coarse_nodes[0, 0]
    weights = coarse_weights[0, 0]

    smem = pl.BlockSpec(memory_space=pltpu.SMEM)
    vmem = pl.BlockSpec(memory_space=pltpu.VMEM)
    hbm = pl.BlockSpec(memory_space=pltpu.HBM)

    def shape(*dims, dtype=F32):
        return jax.ShapeDtypeStruct(dims, dtype)

    def call(kernel, outs, scratch, specs, *args, limit=8):
        args = [
            pltpu.with_memory_space_constraint(arg, pltpu.HBM) if n < len(specs) and specs[n] is hbm else arg
            for n, arg in enumerate(args)
        ]
        return pl.pallas_call(
            kernel,
            out_shape=outs,
            in_specs=specs + [vmem] * (len(args) - len(specs)),
            out_specs=jax.tree.map(lambda _: vmem, outs),
            scratch_shapes=scratch,
            compiler_params=pltpu.CompilerParams(vmem_limit_bytes=limit << 20),
        )(*args)

    field_t = shape(3 * hi, LANES)
    face_t = [shape(3, slots)] * 4
    rows = 3 * local_nodes
    padded = -(-rows // LANES) * LANES
    part_rows = -(-rows // 16) * 16
    lists = local_nodes + 4
    parts_s = [pltpu.VMEM((part_rows, elements), F32)] * 2
    apply_s = [pltpu.VMEM((padded, elements), F32)] + parts_s
    flat_s = pltpu.VMEM((8, nodes_count), F32)
    field_s = pltpu.VMEM((3 * hi, LANES), F32)

    def pairs(axis, parity):
        count = n_grp if axis == 0 else n_dev
        out = []
        for g in range(n_grp):
            for d in range(n_dev):
                here = (g, d)[axis]
                there = here + 1 if here % 2 == parity else here - 1
                if axis == 0:
                    other = (there, d) if 0 <= there < count else (g, d ^ 1)
                else:
                    other = (g, there % count)
                out.append((g * n_dev + d, other[0] * n_dev + other[1]))
        return out

    routes = [pairs(axis, parity) for axis in (0, 1) for parity in (0, 1)]

    def swap(faces_out):
        return [lax.ppermute(face, ("grp", "dev"), route) for face, route in zip(faces_out, routes)]

    diag, *out = call(
        diag_kernel,
        [field_t] + face_t + [
            shape(-(-lists // 8) * 8, elements, dtype=jnp.int32), shape(1, elements), field_t, field_t,
            shape(part_rows, padded, dtype=BF16), shape(part_rows, padded, dtype=BF16),
            shape(lists, LANES, elements, dtype=BF16), shape(lists, hi, elements, dtype=BF16)],
        [pltpu.VMEM(nodes.shape, jnp.int32), pltpu.VMEM(faces.shape, jnp.int32),
         pltpu.VMEM(elem_matrix.shape, F32), pltpu.VMEM((part_rows, padded), F32)] + parts_s
        + [pltpu.SemaphoreType.DMA((6,))],
        [smem] + [hbm] * 6, par, nodes, coef, mass, right, faces, elem_matrix)
    out, (index, coef, mass, right, mat_high, mat_low, low_hot, high_hot) = out[:4], out[4:]
    element = (index, coef, mat_high, mat_low, low_hot, high_hot)

    got = swap(out)

    def prepare(*refs):
        prepare_kernel(width, *refs)

    table = call(
        prepare, shape(2 * WINDOW, nodes_count, dtype=BF16),
        [pltpu.VMEM(coarse.shape, jnp.int32), pltpu.VMEM(weights.shape, F32), pltpu.SemaphoreType.DMA((2,))],
        [smem, hbm, hbm], par, coarse, weights)
    half_rows = chol_inverse.shape[0] // 2
    half_t = [pltpu.VMEM((half_rows, 3 * width), F32)]

    def call_moving(kernel, outs, first_row, *args):
        return call(
            with_move(kernel, len(args), len(outs), first_row), outs + half_t,
            apply_s + [pltpu.SemaphoreType.DMA((CHUNKS,))], [hbm], chol_inverse, *args, limit=BIG)

    gain, field, local, *out, upper = call_moving(
        first_kernel, [field_t] * 3 + face_t, 0, diag, *got, mass, right, *element)
    got = swap(out)
    field, local, *out, lower = call_moving(
        sweep_kernel, [field_t] * 2 + face_t, half_rows, local, *got, field, gain, mass, right, *element)
    got = swap(out)
    window = call(
        restrict_kernel, shape(total, 4, LANES), [field_s, flat_s], [],
        local, *got, right, low_hot, high_hot, table)
    windows = lax.all_to_all(window, ("grp", "dev"), 0, 0)

    def coarse_solve(*refs):
        coarse_kernel(n_dev, width, *refs)

    parts = call(
        coarse_solve, [shape(8, LANES)] * n_dev,
        [pltpu.VMEM((3 * width // LANES, 8, LANES), F32), pltpu.VMEM((chol_inverse.shape[0], LANES), F32)],
        [smem], par, windows, upper, lower)
    corrections = [parts[0]]
    for step in range(1, n_dev):
        corrections.append(lax.ppermute(parts[step], "dev", [(i, i ^ step) for i in range(n_dev)]))

    field, local, *out = call(
        prolong_kernel, [field_t] * 2 + face_t, apply_s + [flat_s, field_s, field_s, field_s], [],
        *corrections, field, table, mass, *element)
    for _ in range(POST - 1):
        got = swap(out)
        field, local, *out = call(
            sweep_kernel, [field_t] * 2 + face_t, apply_s, [], local, *got, field, gain, mass, right, *element)
    got = swap(out)
    field = call(last_kernel, field_t, [], [], local, *got, field, gain, right, low_hot, high_hot)
    return field.reshape(1, 1, 3, nodes_count)


def solution(mesh):
    mesh_shape = (mesh.shape["grp"], mesh.shape["dev"])

    def local(*args):
        return local_program(mesh_shape, *args)

    return jax.shard_map(
        local,
        mesh=mesh,
        in_specs=(
            P("grp", "dev", None, None),
            P("grp", "dev", None, None),
            P("grp", "dev", None),
            P("grp", "dev", None, None),
            P("grp", "dev", None, None),
            P("grp", "dev", None, None),
            P("grp", "dev", None, None),
            P(),
            P("dev", None),
        ),
        out_specs=P("grp", "dev", None, None),
        check_vma=False,
    )
```
